256 devices in a mesh: cfg: 2 (over y), space: 16 (over z), tm: 8 (over x, core).
Axes of the slice: x: 4, y: 2, z: 16, core: 2. Of those that a mesh axis runs over, the one named last changes fastest.
The devices are a block of a 4x16x16 slice.
Arguments:
- solutions: bfloat16 [32, 128, 32, 12288], P(('cfg', 'tm'), None, None, 'space'), parts along dimension 0, may hold values from -6 to 6
- eigvecs: bfloat16 [32, 2, 128, 12288], P(('cfg', 'tm'), None, 'space'), parts along dimension 0, may hold values from -0.0390625 to 0.0390625
- source_time: int32 [256], P('cfg'), parts along dimension 0, may hold values from 0 to 15
Outputs:
- perambulator: bfloat16 [32, 128, 32, 128], P(('cfg', 'tm'), 'space'), parts along dimension 0
The draws below stay inside these ranges and needn't reach their ends.
There are 2 independent parts, one for each index of `cfg`. The reference program is written for one: setup_inputs(seed, part) draws one part's arguments, and reference() takes and returns one part's arrays. A program takes and returns all parts, laid end to end along the dimension named above; each array names one. Nothing has to cross between parts.
All inputs are finite; a program needn't handle non-finite values.
Results may differ from the reference program's by a relative error of at most 0.001.
Values may be sent and summed in bfloat16 or wider, within the bound.
No kernel may reach another device: no remote copies, remote signals or barrier semaphores. Data moves between devices by JAX's collectives and lax.ppermute only.
A program may use at most 128 MiB of HBM per device.

```python
import jax
import jax.numpy as jnp
from jax import lax

NVEC = 128
NSRC = 128
NT = 16
CV = 12288


def place_ends(array, key, low, high):
    extent = array.shape
    spot = [jax.random.randint(jax.random.fold_in(key, axis), (), 0, extent[axis]) for axis in range(len(extent))]
    array = array.at[tuple(spot)].set(low)
    longest = extent.index(max(extent))
    spot[longest] = (spot[longest] + 1) % extent[longest]
    return array.at[tuple(spot)].set(high)


def strengthened(values, key, source, target, blocks, factor):
    owner, partner = [(jnp.arange(values.shape[position]) // (values.shape[position] // blocks)).reshape([-1 if axis == position else 1 for axis in range(values.ndim)]) for position in (source, target)]
    chosen = jax.random.permutation(key, blocks)[partner]
    strong = (owner == chosen) | (owner == (partner + blocks // 2) % blocks)
    return jnp.where(strong, factor * values, values)


def shard_levels(key, dims, cuts, low, high):
    def one(dim, parts):
        steps = jax.random.uniform(jax.random.fold_in(jax.random.fold_in(key, 6), dim), (parts,), jnp.float32, low / len(cuts), high / len(cuts))
        return jnp.repeat(jnp.exp(steps), dims[dim] // parts).reshape((-1,) + (1,) * (len(dims) - dim - 1))

    factor_of = one(*cuts[0])
    for cut in cuts[1:]:
        factor_of = factor_of * one(*cut)
    return factor_of


def gaussian(own_key, extent, width, limit, cuts=(), kind=jnp.bfloat16):
    drawn = width * jax.random.normal(own_key, extent, jnp.float32)
    if cuts:
        drawn = drawn * shard_levels(own_key, extent, cuts, -0.22, 0.18)
    return jnp.clip(drawn, -limit, limit).astype(kind)


def heavy_noise(rng, dims, spread, bound, cuts, heavy, kind=jnp.bfloat16):
    drawn = spread * jax.random.normal(rng, dims, jnp.float32)
    if cuts:
        drawn = drawn * shard_levels(rng, dims, cuts, -0.22, 0.18)
    return jnp.clip(strengthened(drawn, jax.random.fold_in(rng, 3), *heavy), -bound, bound).astype(kind)


def setup_inputs(seed: int = 0, part: int = 0) -> dict:
    key_of = jax.random.split(jax.random.key(seed), 4)
    part_splits = jax.random.split(jax.random.fold_in(key_of[3], part), 4)
    solutions = heavy_noise(part_splits[0], (NT, NSRC, 32, CV), 1.0, 6.0, ((0, 8), (3, 16)), (3, 1, 16, 2.0))
    eigvecs = gaussian(part_splits[1], (NT, 2, NVEC, CV), (2 * CV) ** -0.5, 0.0390625, ((0, 8), (2, 16)))
    source_time = place_ends(jax.random.randint(part_splits[2], (NSRC,), 0, NT), jax.random.fold_in(part_splits[2], 1), 0, NT - 1).astype(jnp.int32)
    return {"solutions": solutions, "eigvecs": eigvecs, "source_time": source_time}


def contract_slice(spinors, vectors):
    sources = spinors.shape[0]
    count = vectors.shape[1]
    stacked = vectors.reshape(2 * count, vectors.shape[2])
    products = jnp.dot(spinors.reshape(sources * 32, spinors.shape[2]), stacked.T, precision=lax.Precision.HIGHEST, preferred_element_type=jnp.float32)
    products = products.reshape(sources, 2, 16, 2, count)
    real_part = products[:, 0, :, 0, :] + products[:, 1, :, 1, :]
    imag_part = products[:, 1, :, 0, :] - products[:, 0, :, 1, :]
    return jnp.concatenate([real_part, imag_part], axis=1)


def reference(solutions, eigvecs, source_time):
    def one_slice(pair):
        return contract_slice(pair[0].astype(jnp.float32), pair[1].astype(jnp.float32))

    sums = lax.map(one_slice, (solutions, eigvecs))
    times = jnp.arange(NT, dtype=jnp.int32)
    signs = jnp.where(times[:, None] < source_time[None, :], -1.0, 1.0).astype(jnp.float32)
    return (sums * signs[:, :, None, None]).astype(jnp.bfloat16)
```

```python
import functools

import jax
import jax.numpy as jnp
from jax import lax
from jax.experimental import pallas as pl
from jax.experimental.pallas import tpu as pltpu
from jax.sharding import PartitionSpec as P

LEVELS = 32766.0
STEPS_PER_OCTAVE = 64.0
LN2 = 0.6931471805599453


def scale_of(code):
    return jnp.exp2(code * (1.0 / STEPS_PER_OCTAVE))


def encode(sums, message_ref, groups, rows):
    largest = jnp.maximum(jnp.max(jnp.abs(sums), axis=1), 1e-30)
    code = jnp.ceil(jnp.log(largest) * (STEPS_PER_OCTAVE / LN2))
    inverse = LEVELS / scale_of(code)
    levels = jnp.round(sums * inverse[:, None, :]).astype(jnp.int32).astype(jnp.int16)
    message_ref[: groups * rows, :] = levels.reshape(groups * rows, levels.shape[2])
    message_ref[groups * rows :, :] = code.astype(jnp.int32).astype(jnp.int16)


def decode(message_ref, groups, rows):
    code = message_ref[groups * rows :, :].astype(jnp.int32).astype(jnp.float32)
    levels = message_ref[: groups * rows, :].astype(jnp.int32).astype(jnp.float32)
    step = scale_of(code) * (1.0 / LEVELS)
    return levels.reshape(groups, rows, levels.shape[1]) * step[:, None, :]


def partial_kernel(owner_ref, spinors_ref, vectors_ref, out_ref):
    slices, sources, rows, sites = spinors_ref.shape
    peers, _, _, own, _ = vectors_ref.shape
    count = peers * own
    half = rows // 2
    for t in range(slices):
        spinors = spinors_ref[t].reshape(sources * rows, sites)
        vectors = jnp.concatenate([vectors_ref[:, t, part].reshape(count, sites) for part in (0, 1)], axis=0)
        products = lax.dot_general(
            spinors, vectors, (((1,), (1,)), ((), ())), preferred_element_type=jnp.float32
        ).reshape(sources, rows, 2 * count)
        real_re = products[:, :half, :count]
        imag_re = products[:, half:, :count]
        real_im = products[:, :half, count:]
        imag_im = products[:, half:, count:]
        out_ref[0, t * sources : (t + 1) * sources, :half, :] = real_re + imag_im
        out_ref[0, t * sources : (t + 1) * sources, half:, :] = imag_re - real_im


def partials(owners, solutions, vectors, sources):
    slices, _, rows, sites = solutions.shape
    count = vectors.shape[0] * vectors.shape[3]
    return pl.pallas_call(
        partial_kernel,
        grid_spec=pltpu.PrefetchScalarGridSpec(
            num_scalar_prefetch=1,
            grid=(owners.shape[0],),
            in_specs=[
                pl.BlockSpec((slices, sources, rows, sites), lambda i, who: (0, who[i], 0, 0)),
                pl.BlockSpec(memory_space=pltpu.VMEM),
            ],
            out_specs=pl.BlockSpec((1, slices * sources, rows, count), lambda i, who: (i, 0, 0, 0)),
        ),
        out_shape=pltpu.VMEM((owners.shape[0], slices * sources, rows, count), jnp.float32),
        cost_estimate=pl.CostEstimate(
            flops=owners.shape[0] * slices * sources * rows * sites * 2 * count * 2,
            bytes_accessed=owners.shape[0] * slices * sources * (rows * sites * 2 + rows * count * 4),
            transcendentals=0,
        ),
    )(owners, solutions, in_vmem(vectors))


def step_kernel(own_ref, *refs, received):
    arms = len(received)
    _, groups, rows, _ = own_ref.shape
    messages, outs = refs[: sum(received)], refs[sum(received) :]
    taken = 0
    for arm in range(arms):
        sums = own_ref[arm]
        if received[arm]:
            sums = sums + decode(messages[taken], groups, rows)
            taken += 1
        encode(sums, outs[arm], groups, rows)


def step(own, messages):
    _, groups, rows, count = own.shape
    arms = len(messages)
    arrived = [m for m in messages if m is not None]
    shape = pltpu.VMEM((groups * (rows + 1), count), jnp.int16)
    return pl.pallas_call(
        functools.partial(step_kernel, received=tuple(m is not None for m in messages)),
        out_shape=[shape] * arms,
        in_specs=[pl.BlockSpec(memory_space=pltpu.VMEM)] * (1 + len(arrived)),
        out_specs=[pl.BlockSpec(memory_space=pltpu.VMEM)] * arms,
    )(in_vmem(own), *map(in_vmem, arrived))


def last_kernel(own_ref, left_ref, right_ref, signs_ref, out_ref):
    _, groups, rows, count = own_ref.shape
    sums = own_ref[0] + decode(left_ref, groups, rows) + decode(right_ref, groups, rows)
    signed = sums * signs_ref[...][:, None, :]
    out_ref[...] = signed.astype(jnp.bfloat16).reshape(out_ref.shape)


def last(own, left, right, signs, slices):
    _, groups, rows, count = own.shape
    return pl.pallas_call(
        last_kernel,
        out_shape=jax.ShapeDtypeStruct((slices, groups // slices, rows, count), jnp.bfloat16),
        in_specs=[pl.BlockSpec(memory_space=pltpu.VMEM)] * 4,
        out_specs=pl.BlockSpec(memory_space=pltpu.VMEM),
    )(in_vmem(own), in_vmem(left), in_vmem(right), in_vmem(signs))


def exchange(eigvecs, devices):
    slices, parts, own, whole = eigvecs.shape
    pieces = jnp.moveaxis(eigvecs.reshape(slices, parts, own, devices, whole // devices), 3, 0)
    return lax.all_to_all(pieces, "space", split_axis=0, concat_axis=0, tiled=True)


def in_vmem(array):
    return pltpu.with_memory_space_constraint(array, pltpu.VMEM)


def shards(solutions, eigvecs, source_time):
    slices = solutions.shape[0]
    devices = lax.axis_size("space")
    sources = solutions.shape[1] // devices
    count = eigvecs.shape[2] * devices
    me = lax.axis_index("space")
    vectors = exchange(eigvecs, devices)

    owned_times = lax.dynamic_slice_in_dim(source_time, me * sources, sources)
    slice_index = lax.axis_index("tm") * slices + jnp.arange(slices, dtype=jnp.int32)
    signs = jnp.where(slice_index[:, None] < owned_times[None, :], -1.0, 1.0).astype(jnp.float32)
    signs = jnp.broadcast_to(signs.reshape(slices * sources, 1), (slices * sources, count))

    ahead = [(i, (i + 1) % devices) for i in range(devices)]
    back = [(i, (i - 1) % devices) for i in range(devices)]
    reach = devices // 2
    offsets = jnp.array([reach] + [s * d for d in range(reach - 1, 0, -1) for s in (1, -1)] + [0], jnp.int32)
    owners = (me + offsets) % devices

    own = partials(owners[:1], solutions, vectors, sources)
    (right,) = step(own, [None])
    right = lax.ppermute(right, "space", ahead)
    left = None
    for k in range(1, reach):
        own = partials(owners[2 * k - 1 : 2 * k + 1], solutions, vectors, sources)
        right, left = step(own, [right, left])
        right = lax.ppermute(right, "space", ahead)
        left = lax.ppermute(left, "space", back)
    own = partials(owners[2 * reach - 1 :], solutions, vectors, sources)
    return last(own, right, left, signs, slices)


def solution(mesh):
    return jax.shard_map(
        shards,
        mesh=mesh,
        in_specs=(
            P(("cfg", "tm"), None, None, "space"),
            P(("cfg", "tm"), None, "space", None),
            P("cfg"),
        ),
        out_specs=P(("cfg", "tm"), "space", None, None),
        check_vma=False,
    )
```
